128 devices in a mesh: gx: 4 (over y_hi, core), gy: 4 (over z), gz: 8 (over y_lo, x).
Axes of the slice: x: 4, y: 4 (y_hi: 2, y_lo: 2; y = y_hi * 2 + y_lo), z: 4, core: 2. Of those that a mesh axis runs over, the one named last changes fastest.
Arguments:
- inputs: bfloat16 [131072, 2048], P(('gx', 'gy', 'gz')), may hold values from -24 to 24
- cotangent: bfloat16 [131072, 4096], P(('gx', 'gy', 'gz')), may hold values from -0.016479492 to 0.016479492
- master: float32 [2048, 4096], P(('gx', 'gy', 'gz')), may hold values from -3 to 3
- accum: float32 [2048, 4096], P(('gx', 'gy', 'gz')), may hold values from 0.05 to 1
Outputs:
- new_master: float32 [2048, 4096], P(('gx', 'gy', 'gz'))
- new_accum: float32 [2048, 4096], P(('gx', 'gy', 'gz'))
The draws below stay inside these ranges and needn't reach their ends.
All inputs are finite; a program needn't handle non-finite values.
Results may differ from the reference program's by a relative error of at most 0.0003.
Values sent between devices are 32-bit elements; how exact they have to be, the bound alone decides.
A program may use at most 128 MiB of HBM per device.

```python
import math
import jax
import jax.numpy as jnp
from jax import lax

D = 4096
ROWS = 2048
TOKENS = 131072


def spiked(drawn, rng, source, target, shards_of, factor):
    owner, partner = [(jnp.arange(drawn.shape[position]) // (drawn.shape[position] // shards_of)).reshape([-1 if axis == position else 1 for axis in range(drawn.ndim)]) for position in (source, target)]
    chosen = jax.random.permutation(rng, shards_of)[partner]
    strong = (owner == chosen) | (owner == (partner + shards_of // 2) % shards_of)
    return jnp.where(strong, factor * drawn, drawn)


def shard_levels(rng, shape, shards, low, high):
    factor_of, own = 1.0, jax.random.fold_in(rng, 6)
    for axis_at, parts in shards:
        steps = jnp.exp(jax.random.uniform(jax.random.fold_in(own, axis_at), (parts,), jnp.float32, low / len(shards), high / len(shards)))
        factor_of = factor_of * jnp.repeat(steps, shape[axis_at] // parts).reshape([-1 if axis == axis_at else 1 for axis in range(len(shape))])
    return factor_of


def bell_draw(stream_key, dims, spread, most, cuts=(), dtype=jnp.bfloat16):
    array = spread * jax.random.normal(stream_key, dims, jnp.float32)
    if cuts:
        array = array * shard_levels(stream_key, dims, cuts, -0.22, 0.18)
    return jnp.clip(array, -most, most).astype(dtype)


def heavy_noise(own_key, dims, width, most, split, heavy, dtype=jnp.bfloat16):
    values = width * jax.random.normal(own_key, dims, jnp.float32)
    if split:
        values = values * shard_levels(own_key, dims, split, -0.22, 0.18)
    return jnp.clip(spiked(values, jax.random.fold_in(own_key, 3), *heavy), -most, most).astype(dtype)


def setup_inputs(seed: int = 0) -> dict:
    key_list = jax.random.split(jax.random.key(seed), 5)
    return {
        "inputs": heavy_noise(key_list[0], (TOKENS, ROWS), 1.0, 24.0, ((0, 128),), (0, 1, 128, 5.5)),
        "cotangent": bell_draw(key_list[1], (TOKENS, D), (TOKENS ** -0.5), 0.016479492, ((0, 128),)),
        "master": bell_draw(key_list[2], (ROWS, D), 0.5, 3.0, ((0, 128),), jnp.float32),
        "accum": jnp.clip(jnp.exp(math.log(1.0) - 2.9957323 * jax.random.uniform(key_list[3], (ROWS, D), jnp.float32) ** shard_levels(key_list[3], (ROWS, D), ((0, 128),), -0.2, 0.2)), 0.05, 1.0),
    }


def reference(inputs, cotangent, master, accum):
    gradient = lax.dot_general(inputs, cotangent, (((0,), (0,)), ((), ())), preferred_element_type=jnp.float32)
    squares = jnp.sum(gradient * gradient)
    limit = 0.5 * jnp.sqrt(jnp.float32(ROWS * D))
    factor = limit / jnp.maximum(jnp.sqrt(squares), limit)
    scaled = factor * gradient
    new_accum = accum + scaled * scaled
    new_master = master - 0.5 * scaled / jnp.sqrt(new_accum)
    return (new_master, new_accum)
```

```python
import jax
import jax.numpy as jnp
from jax import lax
from jax.experimental import pallas as pl
from jax.experimental.pallas import tpu as pltpu
from jax.sharding import PartitionSpec as P

MESH = pl.DeviceIdType.MESH

D = 4096
ROWS = 2048
TOKENS = 1024
W = 128
PORTIONS = 3
WIDE = PORTIONS * W
CHUNKS = 11
LAST = CHUNKS - 1
UNITS = 33
TILE = 256
ORDERS = (("x", "y", "z"), ("y", "z", "x"), ("z", "x", "y"))
COUNTS = (CHUNKS - 1, CHUNKS, CHUNKS)
LAGS = 6


def unit_of(p, k):
    over = k // LAST
    return 3 * k + 2 * over if p == 0 else 3 * k + p - over


def column_of(k):
    return pl.multiple_of((3 * k - k // LAST) * W, W)


def kernel(
    x_hbm, c_hbm, master_hbm, accum_hbm,
    new_master, new_accum,
    xv, xt, cv, stage, other, part, fwd1, got1, fwd2, got2, got3,
    grad, master, accum, squares, norm_out, norm_in,
    x_sem, c_sem, state_sem, stage_sem, other_sem, send_sem,
    fwd1_sem, got1_sem, fwd2_sem, got2_sem, got3_sem, norm_send, norm_recv,
):
    gx, gy, gz = lax.axis_index("gx"), lax.axis_index("gy"), lax.axis_index("gz")
    core = gx % 2
    me = {"x": gz % 4, "y": 2 * (gx // 2) + gz // 4, "z": gy}

    def device(axis=None, step=0, on=None):
        at = dict(me)
        if axis is not None:
            at[axis] = (at[axis] + step) % 4
        on = core if on is None else on
        return (2 * (at["y"] // 2) + on, at["z"], 4 * (at["y"] % 2) + at["x"])

    partner = device(on=1 - core)

    x_loads = []
    for j in range(4):
        whose = 1 - core if j < 2 else core
        at = pl.multiple_of((j % 2) * 1024 + whose * 512, 512)
        x_loads.append(
            pltpu.make_async_copy(x_hbm.at[:, pl.ds(at, 512)], xv.at[j], x_sem.at[j])
        )
    c_first = pltpu.make_async_copy(
        c_hbm.at[:, pl.ds(0, WIDE)], cv.at[:, pl.ds(0, WIDE)], c_sem.at[0]
    )
    c_rest = pltpu.make_async_copy(
        c_hbm.at[:, pl.ds(WIDE, D - WIDE)], cv.at[:, pl.ds(WIDE, D - WIDE)], c_sem.at[1]
    )
    state_loads = [
        pltpu.make_async_copy(master_hbm, master, state_sem.at[0]),
        pltpu.make_async_copy(accum_hbm, accum, state_sem.at[1]),
    ]
    x_loads[0].start()
    c_first.start()
    x_loads[1].start()
    x_loads[2].start()
    x_loads[3].start()

    barrier = pltpu.get_barrier_semaphore()
    pl.semaphore_signal(barrier, inc=1, device_id=partner, device_id_type=MESH)
    for axis in "xyz":
        for step in (1, 2, 3):
            pl.semaphore_signal(
                barrier, inc=1, device_id=device(axis, step), device_id_type=MESH
            )

    squares[...] = jnp.zeros_like(squares)

    def transposed(j):
        for t in range(2):
            xt[2 * j + t] = xv[j, :, t * TILE : (t + 1) * TILE].T

    def product(k, own, store):
        columns = pl.ds(column_of(k), WIDE)

        def tile(m, carry):
            block = jnp.dot(
                xt[4 * own + m], cv[:, columns], preferred_element_type=jnp.float32
            )
            for b in range(16):
                to = {
                    "x": b % 4,
                    "y": 2 * (m // 2) + (b // 4) % 2,
                    "z": 2 * (m % 2) + b // 8,
                }
                rel = {axis: (to[axis] - me[axis] + 4) % 4 for axis in "xyz"}
                for p, (first, second, third) in enumerate(ORDERS):
                    place = 16 * rel[first] + 4 * rel[second] + rel[third]
                    store(p, place, block[16 * b : 16 * b + 16, W * p : W * p + W])
            return carry

        lax.fori_loop(0, 4, tile, 0)

    def exchange(k):
        slot = k % 2

        def store(p, place, value):
            stage[slot, p, place] = value

        product(k, 0, store)
        pltpu.make_async_remote_copy(
            stage.at[slot], other.at[slot], stage_sem.at[slot], other_sem.at[slot],
            device_id=partner, device_id_type=MESH,
        ).start()

    def exchanged(k):
        slot = k % 2
        return pltpu.make_async_remote_copy(
            stage.at[slot], other.at[slot], stage_sem.at[slot], other_sem.at[slot],
            device_id=partner, device_id_type=MESH,
        )

    def send(u, at, size, to, sem, axis, step):
        pltpu.make_async_remote_copy(
            part.at[u, pl.ds(at, size)], to, send_sem.at[u], sem.at[u],
            device_id=device(axis, step), device_id_type=MESH,
        ).start()

    def arrived(u, what, sem):
        pltpu.make_async_remote_copy(
            what.at[u], what.at[u], send_sem.at[u], sem.at[u],
            device_id=partner, device_id_type=MESH,
        ).wait_recv()

    def ring_start(u, axis, size, fwd, fwd_sem, got, got_sem):
        half = size // 2
        send(u, 2 * size, half, fwd.at[u, 0], fwd_sem, axis, 1)
        send(u, 2 * size + half, half, fwd.at[u, 1], fwd_sem, axis, 3)
        send(u, size + half, half, got.at[u, 0, pl.ds(half, half)], got_sem, axis, 1)
        send(u, 3 * size, half, got.at[u, 1, pl.ds(0, half)], got_sem, axis, 3)

    def ring_forward(u, axis, size, fwd, fwd_sem, got, got_sem):
        half = size // 2
        arrived(u, fwd, fwd_sem)
        up, down = pl.ds(size, half), pl.ds(3 * size + half, half)
        part[u, up] = part[u, up] + fwd[u, 0]
        send(u, size, half, got.at[u, 0, pl.ds(0, half)], got_sem, axis, 1)
        part[u, down] = part[u, down] + fwd[u, 1]
        send(u, 3 * size + half, half, got.at[u, 1, pl.ds(half, half)], got_sem, axis, 3)

    def ring_end(u, size, got, got_sem):
        arrived(u, got, got_sem)
        mine = pl.ds(0, size)
        part[u, mine] = part[u, mine] + got[u, 0] + got[u, 1]

    def begin(k):
        slot = k % 2

        def store(p, place, value):
            part[unit_of(p, k), place] = value + other[slot, p, place]

        exchanged(k).wait_recv()
        product(k, 1, store)

    def stages(p, k, lag):
        axes = ORDERS[p]
        u = unit_of(p, k)
        if lag == 0:
            ring_start(u, axes[0], 16, fwd1, fwd1_sem, got1, got1_sem)
        elif lag == 1:
            ring_forward(u, axes[0], 16, fwd1, fwd1_sem, got1, got1_sem)
        elif lag == 2:
            ring_end(u, 16, got1, got1_sem)
            ring_start(u, axes[1], 4, fwd2, fwd2_sem, got2, got2_sem)
        elif lag == 3:
            ring_forward(u, axes[1], 4, fwd2, fwd2_sem, got2, got2_sem)
        elif lag == 4:
            ring_end(u, 4, got2, got2_sem)
            for step in (1, 3, 2):
                send(u, step, 1, got3.at[u, pl.ds(step - 1, 1)], got3_sem, axes[2], step)
        else:
            arrived(u, got3, got3_sem)
            final = part[u, 0] + got3[u, 0] + got3[u, 1] + got3[u, 2]
            grad[:, pl.ds(pl.multiple_of(column_of(k) + W * p, W), W)] = final
            squares[...] = squares[...] + final * final
            pltpu.make_async_remote_copy(
                part.at[u, pl.ds(0, 63)], part.at[u, pl.ds(0, 63)],
                send_sem.at[u], got3_sem.at[u],
                device_id=partner, device_id_type=MESH,
            ).wait_send()

    x_loads[0].wait()
    transposed(0)
    x_loads[1].wait()
    transposed(1)
    c_first.wait()
    product_slot = jnp.int32(0)

    def first_store(p, place, value):
        stage[0, p, place] = value

    product(product_slot, 0, first_store)
    pl.semaphore_wait(barrier, 10)
    exchanged(product_slot).start()
    x_loads[2].wait()
    x_loads[3].wait()
    c_rest.start()
    for load in state_loads:
        load.start()
    transposed(2)
    transposed(3)

    def step(k, carry):
        @pl.when(k < CHUNKS)
        def _():
            begin(k)

        for p in range(PORTIONS):

            @pl.when(k < COUNTS[p])
            def _():
                stages(p, k, 0)

        @pl.when(k == 0)
        def _():
            c_rest.wait()

        @pl.when(k + 1 < CHUNKS)
        def _():
            @pl.when(k >= 1)
            def _():
                exchanged(k - 1).wait_send()

            exchange(k + 1)

        for lag in range(1, LAGS):
            for p in range(PORTIONS):

                @pl.when((k >= lag) & (k - lag < COUNTS[p]))
                def _():
                    stages(p, k - lag, lag)

        return carry

    lax.fori_loop(0, CHUNKS + LAGS - 1, step, 0)
    exchanged(jnp.int32(CHUNKS - 2)).wait_send()
    exchanged(jnp.int32(CHUNKS - 1)).wait_send()

    total = squares[0:8] + squares[8:16]
    for at, axis in enumerate(("core", "x", "y", "z")):
        norm_out[at] = total
        targets = (
            [(0, partner)]
            if axis == "core"
            else [(step - 1, device(axis, step)) for step in (2, 1, 3)]
        )
        copies = [
            pltpu.make_async_remote_copy(
                norm_out.at[at], norm_in.at[at, place], norm_send.at[at, place],
                norm_recv.at[at, place], device_id=target, device_id_type=MESH,
            )
            for place, target in targets
        ]
        for copy in copies:
            copy.start()
        for (place, _), copy in zip(targets, copies):
            copy.wait_recv()
            total = total + norm_in[at, place]
        for copy in copies:
            copy.wait_send()

    limit = 0.5 * jnp.sqrt(jnp.float32(ROWS * D))
    whole = jnp.sum(total, keepdims=True)
    factor = limit / jnp.maximum(jnp.sqrt(whole), limit)
    for load in state_loads:
        load.wait()
    for c in range(0, D, 512):
        columns = slice(c, c + 512)
        scaled = factor * grad[:, columns]
        added = accum[:, columns] + scaled * scaled
        new_accum[:, columns] = added
        new_master[:, columns] = master[:, columns] - 0.5 * scaled / jnp.sqrt(added)


def shards(inputs, cotangent, master, accum):
    vmem, dma = pltpu.VMEM, pltpu.SemaphoreType.DMA
    f32, bf16 = jnp.float32, jnp.bfloat16
    return pl.pallas_call(
        kernel,
        out_shape=(
            jax.ShapeDtypeStruct((16, D), f32),
            jax.ShapeDtypeStruct((16, D), f32),
        ),
        in_specs=[pl.BlockSpec(memory_space=pl.ANY)] * 4,
        out_specs=(pl.BlockSpec(memory_space=vmem), pl.BlockSpec(memory_space=vmem)),
        scratch_shapes=[
            vmem((4, TOKENS, 512), bf16),
            vmem((8, TILE, TOKENS), bf16),
            vmem((TOKENS, D), bf16),
            vmem((2, PORTIONS, 64, 16, W), f32),
            vmem((2, PORTIONS, 64, 16, W), f32),
            vmem((UNITS, 64, 16, W), f32),
            vmem((UNITS, 2, 8, 16, W), f32),
            vmem((UNITS, 2, 16, 16, W), f32),
            vmem((UNITS, 2, 2, 16, W), f32),
            vmem((UNITS, 2, 4, 16, W), f32),
            vmem((UNITS, 3, 16, W), f32),
            vmem((16, D), f32),
            vmem((16, D), f32),
            vmem((16, D), f32),
            vmem((16, W), f32),
            vmem((4, 8, W), f32),
            vmem((4, 3, 8, W), f32),
            dma((4,)),
            dma((2,)),
            dma((2,)),
            dma((2,)),
            dma((2,)),
            dma((UNITS,)),
            dma((UNITS,)),
            dma((UNITS,)),
            dma((UNITS,)),
            dma((UNITS,)),
            dma((UNITS,)),
            dma((4, 3)),
            dma((4, 3)),
        ],
        compiler_params=pltpu.CompilerParams(
            collective_id=0, has_side_effects=True, vmem_limit_bytes=67_043_328
        ),
        name="gradient_step",
    )(inputs, cotangent, master, accum)


def solution(mesh):
    rows = P(("gx", "gy", "gz"), None)
    return jax.shard_map(
        shards, mesh=mesh, in_specs=(rows,) * 4, out_specs=(rows, rows), check_vma=False
    )
```

```python
import jax
import jax.numpy as jnp
from jax import lax
from jax.experimental import pallas as pl
from jax.experimental.pallas import tpu as pltpu
from jax.sharding import PartitionSpec as P

MESH = pl.DeviceIdType.MESH

D = 4096
ROWS = 2048
TOKENS = 1024
W = 128
EACH = 4
WIDE = EACH * W
CHUNKS = D // WIDE
UNITS = D // W
TILE = 512
SLOTS = 4


def one_hot(axis):
    return ((axis + 2) % 3 // 2, (axis + 1) % 3 // 2, axis // 2)


def kernel(
    x_hbm, c_hbm,
    grad_hbm, factor_ref,
    xv, xt, cv, stage, other, part, fwd1, got1, fwd2, got2, got3,
    grad, squares, norm_out, norm_in1, norm_in2,
    x_sem, c_sem, grad_sem, stage_sem, other_sem, send_sem,
    fwd1_sem, got1_sem, fwd2_sem, got2_sem, got3_sem, norm_send, norm_recv,
):
    gx, gy, gz = lax.axis_index("gx"), lax.axis_index("gy"), lax.axis_index("gz")
    core = gx % 2
    me = (gz % 4, 2 * (gx // 2) + gz // 4, gy)

    def device(x, y, z, on):
        return (2 * (y // 2) + on, z, 4 * (y % 2) + x)

    def along(axis, step):
        x, y, z = ((at + step * hot) % 4 for at, hot in zip(me, one_hot(axis)))
        return device(x, y, z, core)

    partner = device(*me, 1 - core)

    x_loads = []
    for j in range(4):
        whose = 1 - core if j < 2 else core
        at = pl.multiple_of((j % 2) * 1024 + whose * 512, 512)
        x_loads.append(
            pltpu.make_async_copy(x_hbm.at[:, pl.ds(at, 512)], xv.at[j], x_sem.at[j])
        )
    c_first = pltpu.make_async_copy(
        c_hbm.at[:, pl.ds(0, WIDE)], cv.at[:, pl.ds(0, WIDE)], c_sem.at[0]
    )
    c_rest = pltpu.make_async_copy(
        c_hbm.at[:, pl.ds(WIDE, D - WIDE)], cv.at[:, pl.ds(WIDE, D - WIDE)], c_sem.at[1]
    )
    x_loads[0].start()
    c_first.start()
    x_loads[1].start()
    x_loads[2].start()
    x_loads[3].start()

    column = [
        (3 * on + step - 1, (me[0], me[1], (me[2] + step) % 4), (core + on) % 2)
        for step, on in ((2, 1), (2, 0), (1, 1), (3, 1), (1, 0), (3, 0), (4, 1))
    ]
    column = [(place, device(*at, on)) for place, at, on in column]
    plane = [
        (4 * a + b - 1 - (a > 0), device((me[0] + a) % 4, (me[1] + b) % 4, me[2], core))
        for a in (2, 1, 3, 0)
        for b in (2, 1, 3, 4)
        if (a, b) != (0, 4)
    ]
    barrier = pltpu.get_barrier_semaphore()
    for _, target in column + plane:
        pl.semaphore_signal(barrier, inc=1, device_id=target, device_id_type=MESH)

    squares[...] = jnp.zeros_like(squares)

    def transposed(j):
        xt[j] = xv[j].T

    def product(k, own, store):
        columns = pl.ds(pl.multiple_of(k * WIDE, WIDE), WIDE)
        hots = [one_hot((EACH * k + j) % 3) for j in range(EACH)]
        weights = [
            (16 * a + b + 4 * c, 4 * a + 16 * b + c, a + 4 * b + 16 * c)
            for a, b, c in hots
        ]

        def tile(m, carry):
            block = jnp.dot(
                xt[2 * own + m], cv[:, columns], preferred_element_type=jnp.float32
            )
            for j in range(EACH):
                wx, wy, wz = weights[j]
                xs = [wx * ((to - me[0] + 4) % 4) for to in range(4)]
                ys = [wy * ((2 * m + to - me[1] + 4) % 4) for to in range(2)]
                zs = [wz * ((to - me[2] + 4) % 4) for to in range(4)]
                for b in range(32):
                    place = xs[b % 4] + ys[b // 4 % 2] + zs[b // 8]
                    store(j, place, block[16 * b : 16 * b + 16, W * j : W * j + W])
            return carry

        lax.fori_loop(0, 2, tile, 0)

    def exchanged(k, j):
        slot, to = k % 2, k % SLOTS
        return pltpu.make_async_remote_copy(
            stage.at[slot, j], other.at[to, j], stage_sem.at[slot], other_sem.at[to, j],
            device_id=partner, device_id_type=MESH,
        )

    def exchange_product(k):
        def store(j, place, value):
            stage[k % 2, j, place] = value

        product(k, 0, store)

    def exchange(k):
        for j in range(EACH):
            exchanged(k, j).start()

    def exchange_sent(k):
        slot = k % 2
        pltpu.make_async_remote_copy(
            stage.at[slot], other.at[0], stage_sem.at[slot], other_sem.at[0, 0],
            device_id=partner, device_id_type=MESH,
        ).wait_send()

    def send(u, at, size, to, sem, target):
        pltpu.make_async_remote_copy(
            part.at[u, pl.ds(at, size)], to, send_sem.at[u], sem.at[u],
            device_id=target, device_id_type=MESH,
        ).start()

    def arrived(u, what, sem):
        pltpu.make_async_remote_copy(
            what.at[u], what.at[u], send_sem.at[u], sem.at[u],
            device_id=partner, device_id_type=MESH,
        ).wait_recv()

    def ring_start(u, axis, size, fwd, fwd_sem, got, got_sem):
        half = size // 2
        up, down = along(axis, 1), along(axis, 3)
        send(u, 2 * size, half, fwd.at[u, 0], fwd_sem, up)
        send(u, 2 * size + half, half, fwd.at[u, 1], fwd_sem, down)
        send(u, size + half, half, got.at[u, 0, pl.ds(half, half)], got_sem, up)
        send(u, 3 * size, half, got.at[u, 1, pl.ds(0, half)], got_sem, down)

    def ring_forward(u, axis, size, fwd, fwd_sem, got, got_sem):
        half = size // 2
        arrived(u, fwd, fwd_sem)
        up, down = pl.ds(size, half), pl.ds(3 * size + half, half)
        part[u, up] = part[u, up] + fwd[u, 0]
        part[u, down] = part[u, down] + fwd[u, 1]
        send(u, size, half, got.at[u, 0, pl.ds(0, half)], got_sem, along(axis, 1))
        send(u, 3 * size + half, half, got.at[u, 1, pl.ds(half, half)], got_sem, along(axis, 3))

    def ring_end(u, size, got, got_sem):
        arrived(u, got, got_sem)
        mine = pl.ds(0, size)
        part[u, mine] = part[u, mine] + got[u, 0] + got[u, 1]

    def start1(u):
        ring_start(u, u % 3, 16, fwd1, fwd1_sem, got1, got1_sem)

    def forward1(u):
        ring_forward(u, u % 3, 16, fwd1, fwd1_sem, got1, got1_sem)

    def start2(u):
        ring_end(u, 16, got1, got1_sem)
        ring_start(u, (u + 1) % 3, 4, fwd2, fwd2_sem, got2, got2_sem)

    def forward2(u):
        ring_forward(u, (u + 1) % 3, 4, fwd2, fwd2_sem, got2, got2_sem)

    def start3(u):
        ring_end(u, 4, got2, got2_sem)
        for step in (2, 1, 3):
            send(u, step, 1, got3.at[u, pl.ds(step - 1, 1)], got3_sem, along((u + 2) % 3, step))

    def end3(u):
        arrived(u, got3, got3_sem)
        final = part[u, 0] + got3[u, 0] + got3[u, 1] + got3[u, 2]
        grad[:, pl.ds(pl.multiple_of(u * W, W), W)] = final
        squares[...] = squares[...] + final * final
        pltpu.make_async_remote_copy(
            part.at[u, pl.ds(0, 63)], part.at[u, pl.ds(0, 63)],
            send_sem.at[u], got3_sem.at[u],
            device_id=partner, device_id_type=MESH,
        ).wait_send()

    def each(k, what):
        for j in range(EACH):
            what(EACH * k + j)

    zero, one = jnp.int32(0), jnp.int32(1)
    x_loads[0].wait()
    transposed(0)
    x_loads[1].wait()
    transposed(1)
    c_first.wait()
    exchange_product(zero)
    pl.semaphore_wait(barrier, 22)
    exchange(zero)
    x_loads[2].wait()
    transposed(2)
    x_loads[3].wait()
    transposed(3)
    c_rest.start()

    def first_store(j, place, value):
        part[j, place] = value

    product(zero, 1, first_store)
    for j in range(EACH):
        if j == 2:
            c_rest.wait()
            exchange_product(one)
            exchange(one)
        exchanged(zero, j).wait_recv()

        def add(i, carry, j=j):
            at = pl.ds(8 * i, 8)
            part[j, at] = part[j, at] + other[0, j, at]
            return carry

        lax.fori_loop(0, 8, add, 0)
        start1(jnp.int32(j))
    exchange_sent(zero)
    exchange_product(jnp.int32(2))
    exchange(jnp.int32(2))

    def step(k, carry):
        slot = k % SLOTS

        def store(j, place, value):
            part[EACH * k + j, place] = value + other[slot, j, place]

        for j in range(EACH):
            exchanged(k, j).wait_recv()
        product(k, 1, store)
        each(k, start1)

        @pl.when(k + 2 < CHUNKS)
        def _():
            exchange_sent(k)
            exchange_product(k + 2)
            exchange(k + 2)

        each(k - 1, forward1)

        @pl.when(k >= 3)
        def _():
            each(k - 3, start2)

        @pl.when(k >= 4)
        def _():
            each(k - 4, forward2)

        return carry

    lax.fori_loop(1, CHUNKS, step, 0)
    exchange_sent(CHUNKS - 2)
    exchange_sent(CHUNKS - 1)

    def all_of(low, high, what):
        def one_unit(u, carry):
            what(u)
            return carry

        lax.fori_loop(EACH * low, EACH * high, one_unit, 0)

    all_of(5, 6, start2)
    all_of(4, 5, forward2)
    all_of(7, 8, forward1)
    all_of(6, 7, start2)
    all_of(5, 6, forward2)
    all_of(0, 2, start3)
    all_of(7, 8, start2)
    all_of(6, 7, forward2)
    all_of(2, 4, start3)
    all_of(7, 8, forward2)
    all_of(4, 7, start3)
    all_of(0, 4, end3)
    all_of(7, 8, start3)
    all_of(4, 8, end3)

    to_hbm = pltpu.make_async_copy(grad, grad_hbm, grad_sem)
    to_hbm.start()

    total = squares[0:8] + squares[8:16]
    for level, (targets, inbox) in enumerate(((column, norm_in1), (plane, norm_in2))):
        norm_out[level] = total
        copies = [
            pltpu.make_async_remote_copy(
                norm_out.at[level], inbox.at[place], norm_send.at[level],
                norm_recv.at[level], device_id=target, device_id_type=MESH,
            )
            for place, target in targets
        ]
        for copy in copies:
            copy.start()
        whole = pltpu.make_async_remote_copy(
            inbox, inbox, norm_send.at[level], norm_recv.at[level],
            device_id=partner, device_id_type=MESH,
        )
        whole.wait_recv()
        for place, _ in targets:
            total = total + inbox[place]
        whole.wait_send()

    limit = 0.5 * jnp.sqrt(jnp.float32(ROWS * D))
    whole = jnp.sum(total, keepdims=True)
    factor = limit / jnp.maximum(jnp.sqrt(whole), limit)
    factor_ref[...] = jnp.broadcast_to(factor, factor_ref.shape)
    to_hbm.wait()


def shards(inputs, cotangent, master, accum):
    vmem, dma = pltpu.VMEM, pltpu.SemaphoreType.DMA
    f32, bf16 = jnp.float32, jnp.bfloat16
    gradient, factor = pl.pallas_call(
        kernel,
        out_shape=(
            jax.ShapeDtypeStruct((16, D), f32),
            jax.ShapeDtypeStruct((8, W), f32),
        ),
        in_specs=[pl.BlockSpec(memory_space=pl.ANY)] * 2,
        out_specs=(pl.BlockSpec(memory_space=pl.ANY), pl.BlockSpec(memory_space=vmem)),
        scratch_shapes=[
            vmem((4, TOKENS, 512), bf16),
            vmem((4, TILE, TOKENS), bf16),
            vmem((TOKENS, D), bf16),
            vmem((2, EACH, 64, 16, W), f32),
            vmem((SLOTS, EACH, 64, 16, W), f32),
            vmem((UNITS, 64, 16, W), f32),
            vmem((UNITS, 2, 8, 16, W), f32),
            vmem((UNITS, 2, 16, 16, W), f32),
            vmem((UNITS, 2, 2, 16, W), f32),
            vmem((UNITS, 2, 4, 16, W), f32),
            vmem((UNITS, 3, 16, W), f32),
            vmem((16, D), f32),
            vmem((16, W), f32),
            vmem((2, 8, W), f32),
            vmem((7, 8, W), f32),
            vmem((15, 8, W), f32),
            dma((4,)),
            dma((2,)),
            dma,
            dma((2,)),
            dma((SLOTS, EACH)),
            dma((UNITS,)),
            dma((UNITS,)),
            dma((UNITS,)),
            dma((UNITS,)),
            dma((UNITS,)),
            dma((UNITS,)),
            dma((2,)),
            dma((2,)),
        ],
        compiler_params=pltpu.CompilerParams(
            collective_id=0, has_side_effects=True, vmem_limit_bytes=67_043_328
        ),
        name="gradient_sum",
    )(inputs, cotangent)
    scaled = factor[0, 0] * gradient
    new_accum = accum + scaled * scaled
    new_master = master - 0.5 * scaled / jnp.sqrt(new_accum)
    return new_master, new_accum


def solution(mesh):
    rows = P(("gx", "gy", "gz"), None)
    return jax.shard_map(
        shards, mesh=mesh, in_specs=(rows,) * 4, out_specs=(rows, rows), check_vma=False
    )
```

```python
import jax
import jax.numpy as jnp
from jax import lax
from jax.experimental import pallas as pl
from jax.experimental.pallas import tpu as pltpu
from jax.sharding import PartitionSpec as P

MESH = pl.DeviceIdType.MESH

D = 4096
ROWS = 2048
TOKENS = 1024
W = 128
EACH = 4
WIDE = EACH * W
CHUNKS = D // WIDE
UNITS = D // W
TILE = 512
SLOTS = 4
SENT = 8


def one_hot(axis):
    return ((axis + 2) % 3 // 2, (axis + 1) % 3 // 2, axis // 2)


def kernel(
    x_hbm, c_hbm,
    scaled_hbm,
    xv, xt, cv, stage, other, part, fwd1, got1, fwd2, got2, got3,
    grad, squares, norm_out, norm_in1, norm_in2,
    x_sem, c_sem, grad_sem, stage_sem, other_sem, send_sem,
    fwd1_sem, got1_sem, fwd2_sem, got2_sem, got3_sem, norm_send, norm_recv,
):
    gx, gy, gz = lax.axis_index("gx"), lax.axis_index("gy"), lax.axis_index("gz")
    core = gx % 2
    me = (gz % 4, 2 * (gx // 2) + gz // 4, gy)

    def device(x, y, z, on):
        return (2 * (y // 2) + on, z, 4 * (y % 2) + x)

    def along(axis, step):
        x, y, z = ((at + step * hot) % 4 for at, hot in zip(me, one_hot(axis)))
        return device(x, y, z, core)

    partner = device(*me, 1 - core)

    x_loads = []
    for j in range(4):
        whose = 1 - core if j < 2 else core
        at = pl.multiple_of((j % 2) * 1024 + whose * 512, 512)
        x_loads.append(
            pltpu.make_async_copy(x_hbm.at[:, pl.ds(at, 512)], xv.at[j], x_sem.at[j])
        )
    c_first = pltpu.make_async_copy(
        c_hbm.at[:, pl.ds(0, WIDE)], cv.at[:, pl.ds(0, WIDE)], c_sem.at[0]
    )
    c_second = pltpu.make_async_copy(
        c_hbm.at[:, pl.ds(WIDE, WIDE)], cv.at[:, pl.ds(WIDE, WIDE)], c_sem.at[1]
    )
    rest = pl.ds(2 * WIDE, D - 2 * WIDE)
    c_rest = pltpu.make_async_copy(c_hbm.at[:, rest], cv.at[:, rest], c_sem.at[2])
    x_loads[0].start()
    x_loads[1].start()
    c_first.start()

    column = [
        (3 * on + step - 1, (me[0], me[1], (me[2] + step) % 4), (core + on) % 2)
        for step, on in ((2, 1), (2, 0), (1, 1), (3, 1), (1, 0), (3, 0), (4, 1))
    ]
    column = [(place, device(*at, on)) for place, at, on in column]
    plane = [
        (4 * a + b - 1 - (a > 0), device((me[0] + a) % 4, (me[1] + b) % 4, me[2], core))
        for a in (2, 1, 3, 0)
        for b in (2, 1, 3, 4)
        if (a, b) != (0, 4)
    ]
    barrier = pltpu.get_barrier_semaphore()
    for _, target in column + plane:
        pl.semaphore_signal(barrier, inc=1, device_id=target, device_id_type=MESH)

    squares[...] = jnp.zeros_like(squares)

    def transposed(j):
        xt[j] = xv[j].T

    def product(k, own, store, js=range(EACH)):
        at = pl.multiple_of(k * WIDE + js[0] * W, len(js) * W)
        columns = pl.ds(at, len(js) * W)
        hots = [one_hot((EACH * k + j) % 3) for j in js]
        weights = [
            (32 * a + 2 * b + 8 * c, 8 * a + 32 * b + 2 * c, 2 * a + 8 * b + 32 * c)
            for a, b, c in hots
        ]

        def tile(m, carry):
            block = jnp.dot(
                xt[2 * own + m], cv[:, columns], preferred_element_type=jnp.float32
            )
            for i, j in enumerate(js):
                wx, wy, wz = weights[i]
                xs = [wx * ((to - me[0] + 4) % 4) for to in range(4)]
                ys = [wy * ((2 * m + to - me[1] + 4) % 4) for to in range(2)]
                zs = [wz * ((to - me[2] + 4) % 4) for to in range(4)]
                for b in range(32):
                    place = xs[b % 4] + ys[b // 4 % 2] + zs[b // 8]
                    value = block[16 * b : 16 * b + 16, W * i : W * i + W]
                    store(j, pl.ds(place, 2), value.reshape(2, 8, W))
            return carry

        lax.fori_loop(0, 2, tile, 0)

    def exchanged(k, j):
        slot, to = k % 2, k % SLOTS
        return pltpu.make_async_remote_copy(
            stage.at[slot, j], other.at[to, j], stage_sem.at[slot], other_sem.at[to, j],
            device_id=partner, device_id_type=MESH,
        )

    def exchange_product(k, js=range(EACH)):
        def store(j, place, value):
            stage[k % 2, j, place] = value

        product(k, 0, store, js)

    def exchange(k, js=range(EACH)):
        for j in js:
            exchanged(k, j).start()

    def exchange_sent(k):
        slot = k % 2
        pltpu.make_async_remote_copy(
            stage.at[slot], other.at[0], stage_sem.at[slot], other_sem.at[0, 0],
            device_id=partner, device_id_type=MESH,
        ).wait_send()

    def send(u, at, size, to, sem, target):
        pltpu.make_async_remote_copy(
            part.at[u, pl.ds(at, size)], to, send_sem.at[u // SENT], sem,
            device_id=target, device_id_type=MESH,
        ).start()

    def arrived(u, what, sem):
        pltpu.make_async_remote_copy(
            what.at[u], what.at[u], send_sem.at[0], sem,
            device_id=partner, device_id_type=MESH,
        ).wait_recv()

    def ring_start(u, axis, size, fwd, fwd_sem, got, got_sem):
        half = size // 2
        up, down = along(axis, 1), along(axis, 3)
        send(u, 2 * size, half, fwd.at[u, 0], fwd_sem, up)
        send(u, 2 * size + half, half, fwd.at[u, 1], fwd_sem, down)
        send(u, size + half, half, got.at[u, 0, pl.ds(half, half)], got_sem, up)
        send(u, 3 * size, half, got.at[u, 1, pl.ds(0, half)], got_sem, down)

    def ring_forward(u, axis, size, fwd, got, got_sem):
        half = size // 2
        up, down = pl.ds(size, half), pl.ds(3 * size + half, half)
        part[u, up] = part[u, up] + fwd[u, 0]
        part[u, down] = part[u, down] + fwd[u, 1]
        to_up, to_down = got.at[u, 0, pl.ds(0, half)], got.at[u, 1, pl.ds(half, half)]
        send(u, size, half, to_up, got_sem, along(axis, 1))
        send(u, 3 * size + half, half, to_down, got_sem, along(axis, 3))

    def ring_end(u, size, got):
        mine = pl.ds(0, size)
        part[u, mine] = part[u, mine] + got[u, 0] + got[u, 1]

    def chunk_arrived(k, what, sem):
        units = pl.ds(EACH * k, EACH)
        pltpu.make_async_remote_copy(
            what.at[units], what.at[units], send_sem.at[0], sem.at[k],
            device_id=partner, device_id_type=MESH,
        ).wait_recv()

    def units_of(k):
        return [EACH * k + j for j in range(EACH)]

    def start1(u):
        ring_start(u, u % 3, 32, fwd1, fwd1_sem.at[u], got1, got1_sem.at[u])

    def forward1(k, js=range(EACH)):
        for j in js:
            u = EACH * k + j
            arrived(u, fwd1, fwd1_sem.at[u])
            ring_forward(u, u % 3, 32, fwd1, got1, got1_sem.at[u])

    def start2(k):
        for u in units_of(k):
            arrived(u, got1, got1_sem.at[u])
            ring_end(u, 32, got1)
            ring_start(u, (u + 1) % 3, 8, fwd2, fwd2_sem.at[k], got2, got2_sem.at[k])

    def forward2(k):
        chunk_arrived(k, fwd2, fwd2_sem)
        for u in units_of(k):
            ring_forward(u, (u + 1) % 3, 8, fwd2, got2, got2_sem.at[k])

    def start3(k):
        chunk_arrived(k, got2, got2_sem)
        for u in units_of(k):
            ring_end(u, 8, got2)
            for step in (2, 1, 3):
                to = got3.at[u, step - 1]
                send(u, 2 * step, 2, to, got3_sem.at[k], along((u + 2) % 3, step))

    def end3(k):
        chunk_arrived(k, got3, got3_sem)
        for u in units_of(k):
            final = part[u, 0:2] + got3[u, 0] + got3[u, 1] + got3[u, 2]
            grad[:, pl.ds(pl.multiple_of(u * W, W), W)] = final.reshape(16, W)
            squares[...] = squares[...] + final * final

    def all_sent(i):
        sent = part.at[pl.ds(SENT * i, SENT), pl.ds(0, 126)]
        pltpu.make_async_remote_copy(
            sent, sent, send_sem.at[i], got3_sem.at[0],
            device_id=partner, device_id_type=MESH,
        ).wait_send()

    def own(k, js=range(EACH)):
        def store(j, place, value):
            part[EACH * k + j, place] = value

        product(k, 1, store, js)

    def exchange_ended(k, j):
        u, slot = EACH * k + j, k % SLOTS
        exchanged(k, j).wait_recv()

        def add(i, carry):
            at = pl.ds(pl.multiple_of(16 * i, 16), 16)
            part[u, at] = part[u, at] + other[slot, j, at]
            return carry

        lax.fori_loop(0, 8, add, 0)
        start1(u)

    low, high = range(2), range(2, 4)
    x_loads[0].wait()
    x_loads[2].start()
    x_loads[3].start()
    transposed(0)
    x_loads[1].wait()
    c_second.start()
    transposed(1)
    c_first.wait()
    exchange_product(0, low)
    pl.semaphore_wait(barrier, 22)
    exchange(0, low)
    exchange_product(0, high)
    exchange(0, high)
    x_loads[2].wait()
    transposed(2)
    x_loads[3].wait()
    transposed(3)
    c_second.wait()
    c_rest.start()
    own(0, low)
    exchange_ended(0, 0)
    exchange_ended(0, 1)
    own(0, high)
    exchange_ended(0, 2)
    exchange_ended(0, 3)
    exchange_product(1)
    exchange(1)
    own(1)
    forward1(0, low)
    exchange_ended(1, 0)
    exchange_ended(1, 1)
    forward1(0, high)
    c_rest.wait()
    exchange_sent(0)
    exchange_product(2)
    exchange(2)
    exchange_ended(1, 2)
    exchange_ended(1, 3)

    def step(k, carry):
        own(k)
        for j in range(EACH):
            exchange_ended(k, j)

        @pl.when(k == 2)
        def _():
            exchange_sent(1)
            exchange_product(3)
            exchange(3)

        forward1(k - 1)

        @pl.when(k + 2 < CHUNKS)
        def _():
            exchange_sent(k)
            exchange_product(k + 2)
            exchange(k + 2)

        @pl.when(k < 5)
        def _():
            start2(k - 2)

        @pl.when((k >= 4) & (k < 5))
        def _():
            forward2(k - 4)

        return carry

    lax.fori_loop(2, CHUNKS, step, 0)
    exchange_sent(CHUNKS - 2)
    exchange_sent(CHUNKS - 1)

    def all_of(low, high, what):
        if high - low == 1:
            what(low)
            return

        def one_chunk(k, carry):
            what(k)
            return carry

        lax.fori_loop(low, high, one_chunk, 0)

    all_of(7, 8, forward1)
    all_of(3, 6, start2)
    all_of(1, 3, forward2)
    all_of(6, 8, start2)
    all_of(3, 6, forward2)
    all_of(6, 8, forward2)
    all_of(0, 6, start3)
    all_of(6, 8, start3)
    all_of(0, 8, end3)

    total = squares[0] + squares[1]
    for level, (targets, inbox) in enumerate(((column, norm_in1), (plane, norm_in2))):
        norm_out[level] = total
        copies = [
            pltpu.make_async_remote_copy(
                norm_out.at[level], inbox.at[place], norm_send.at[level],
                norm_recv.at[level], device_id=target, device_id_type=MESH,
            )
            for place, target in targets
        ]
        for copy in copies:
            copy.start()
        whole = pltpu.make_async_remote_copy(
            inbox, inbox, norm_send.at[level], norm_recv.at[level],
            device_id=partner, device_id_type=MESH,
        )
        whole.wait_recv()
        for place, _ in targets:
            total = total + inbox[place]
        whole.wait_send()

    limit = 0.5 * jnp.sqrt(jnp.float32(ROWS * D))
    whole = jnp.sum(total, keepdims=True)
    factor = limit / jnp.maximum(jnp.sqrt(whole), limit)
    grad[...] = grad[...] * factor
    to_hbm = pltpu.make_async_copy(grad, scaled_hbm, grad_sem)
    to_hbm.start()
    for i in range(UNITS // SENT):
        all_sent(i)
    to_hbm.wait()


def shards(inputs, cotangent, master, accum):
    vmem, dma = pltpu.VMEM, pltpu.SemaphoreType.DMA
    f32, bf16 = jnp.float32, jnp.bfloat16
    scaled = pl.pallas_call(
        kernel,
        out_shape=jax.ShapeDtypeStruct((16, D), f32),
        in_specs=[pl.BlockSpec(memory_space=pl.ANY)] * 2,
        out_specs=pl.BlockSpec(memory_space=pl.ANY),
        scratch_shapes=[
            vmem((4, TOKENS, 512), bf16),
            vmem((4, TILE, TOKENS), bf16),
            vmem((TOKENS, D), bf16),
            vmem((2, EACH, 128, 8, W), f32),
            vmem((SLOTS, EACH, 128, 8, W), f32),
            vmem((UNITS, 128, 8, W), f32),
            vmem((UNITS, 2, 16, 8, W), f32),
            vmem((UNITS, 2, 32, 8, W), f32),
            vmem((UNITS, 2, 4, 8, W), f32),
            vmem((UNITS, 2, 8, 8, W), f32),
            vmem((UNITS, 3, 2, 8, W), f32),
            vmem((16, D), f32),
            vmem((2, 8, W), f32),
            vmem((2, 8, W), f32),
            vmem((7, 8, W), f32),
            vmem((15, 8, W), f32),
            dma((4,)),
            dma((3,)),
            dma,
            dma((2,)),
            dma((SLOTS, EACH)),
            dma((UNITS // SENT,)),
            dma((UNITS,)),
            dma((UNITS,)),
            dma((CHUNKS,)),
            dma((CHUNKS,)),
            dma((CHUNKS,)),
            dma((2,)),
            dma((2,)),
        ],
        compiler_params=pltpu.CompilerParams(
            collective_id=0, has_side_effects=True, vmem_limit_bytes=64_000_000
        ),
        name="gradient_sum",
    )(inputs, cotangent)
    new_accum = accum + scaled * scaled
    new_master = master - 0.5 * scaled / jnp.sqrt(new_accum)
    return new_master, new_accum


def solution(mesh):
    rows = P(("gx", "gy", "gz"), None)
    return jax.shard_map(
        shards, mesh=mesh, in_specs=(rows,) * 4, out_specs=(rows, rows), check_vma=False
    )
```

```python
import jax
import jax.numpy as jnp
from jax import lax
from jax.experimental import pallas as pl
from jax.experimental.pallas import tpu as pltpu
from jax.sharding import PartitionSpec as P

MESH = pl.DeviceIdType.MESH

D = 4096
ROWS = 2048
TOKENS = 1024
W = 128
EACH = 4
WIDE = EACH * W
CHUNKS = D // WIDE
UNITS = D // W
TILE = 512
SLOTS = 4
SENT = 8


def one_hot(axis):
    return ((axis + 2) % 3 // 2, (axis + 1) % 3 // 2, axis // 2)


def axes_of(u):
    first = u % 3
    spare = u // 8 % 2 * (1 - u // 16) * one_hot(first)[0]
    return first, (first + 1 + spare) % 3, (first + 2 - spare) % 3


def kernel(
    x_hbm, c_hbm,
    scaled_ref,
    xv, xt, cv, stage, other, part, fwd1, got1, fwd2, got2, got3,
    grad, squares, norm_out, norm_in1, norm_in2,
    x_sem, c_sem, stage_sem, other_sem, send_sem,
    fwd1_sem, got1_sem, fwd2_sem, got2_sem, got3_sem, norm_send, norm_recv,
):
    gx, gy, gz = lax.axis_index("gx"), lax.axis_index("gy"), lax.axis_index("gz")
    core = gx % 2
    me = (gz % 4, 2 * (gx // 2) + gz // 4, gy)

    def device(x, y, z, on):
        return (2 * (y // 2) + on, z, 4 * (y % 2) + x)

    def along(axis, step):
        x, y, z = ((at + step * hot) % 4 for at, hot in zip(me, one_hot(axis)))
        return device(x, y, z, core)

    partner = device(*me, 1 - core)

    x_loads = []
    for j in range(4):
        whose = 1 - core if j < 2 else core
        at = pl.multiple_of((j % 2) * 1024 + whose * 512, 512)
        x_loads.append(
            pltpu.make_async_copy(x_hbm.at[:, pl.ds(at, 512)], xv.at[j % 2], x_sem.at[j])
        )
    c_first, c_next = [
        pltpu.make_async_copy(c_hbm.at[:, at], cv.at[:, at], c_sem.at[i])
        for i, at in ((0, pl.ds(0, 2 * W)), (3, pl.ds(2 * W, 2 * W)))
    ]
    c_second = pltpu.make_async_copy(
        c_hbm.at[:, pl.ds(WIDE, WIDE)], cv.at[:, pl.ds(WIDE, WIDE)], c_sem.at[1]
    )
    rest = pl.ds(2 * WIDE, D - 2 * WIDE)
    c_rest = pltpu.make_async_copy(c_hbm.at[:, rest], cv.at[:, rest], c_sem.at[2])
    x_loads[0].start()
    c_first.start()
    x_loads[1].start()

    column = [
        (3 * on + step - 1, (me[0], me[1], (me[2] + step) % 4), (core + on) % 2)
        for step, on in ((2, 1), (2, 0), (1, 1), (3, 1), (1, 0), (3, 0), (4, 1))
    ]
    column = [(place, device(*at, on)) for place, at, on in column]
    plane = [
        (4 * a + b - 1 - (a > 0), device((me[0] + a) % 4, (me[1] + b) % 4, me[2], core))
        for a in (2, 1, 3, 0)
        for b in (2, 1, 3, 4)
        if (a, b) != (0, 4)
    ]
    barrier = pltpu.get_barrier_semaphore()
    for _, target in column + plane:
        pl.semaphore_signal(barrier, inc=1, device_id=target, device_id_type=MESH)

    squares[...] = jnp.zeros_like(squares)

    def transposed(j):
        xt[j] = xv[j % 2].T

    def product(k, own, store, js=range(EACH)):
        at = pl.multiple_of(k * WIDE + js[0] * W, len(js) * W)
        columns = pl.ds(at, len(js) * W)
        hots = [[one_hot(axis) for axis in axes_of(EACH * k + j)] for j in js]
        weights = [
            [32 * a + 8 * b + 2 * c for a, b, c in zip(*of_unit)] for of_unit in hots
        ]

        def tile(m, carry):
            block = jnp.dot(
                xt[2 * own + m], cv[:, columns], preferred_element_type=jnp.float32
            )
            for i, j in enumerate(js):
                wx, wy, wz = weights[i]
                xs = [wx * ((to - me[0] + 4) % 4) for to in range(4)]
                ys = [wy * ((2 * m + to - me[1] + 4) % 4) for to in range(2)]
                zs = [wz * ((to - me[2] + 4) % 4) for to in range(4)]
                for b in range(32):
                    place = xs[b % 4] + ys[b // 4 % 2] + zs[b // 8]
                    value = block[16 * b : 16 * b + 16, W * i : W * i + W]
                    store(j, pl.ds(place, 2), value.reshape(2, 8, W))
            return carry

        lax.fori_loop(0, 2, tile, 0, unroll=len(js) < EACH)

    def exchanged(k, j):
        slot, to = k % 2, k % SLOTS
        return pltpu.make_async_remote_copy(
            stage.at[slot, j], other.at[to, j], stage_sem.at[slot], other_sem.at[to, j],
            device_id=partner, device_id_type=MESH,
        )

    def exchange_product(k, js=range(EACH)):
        def store(j, place, value):
            stage[k % 2, j, place] = value

        product(k, 0, store, js)

    def exchange(k, js=range(EACH)):
        for j in js:
            exchanged(k, j).start()

    def exchange_sent(k):
        slot = k % 2
        pltpu.make_async_remote_copy(
            stage.at[slot], other.at[0], stage_sem.at[slot], other_sem.at[0, 0],
            device_id=partner, device_id_type=MESH,
        ).wait_send()

    def send(u, at, size, to, sem, target):
        pltpu.make_async_remote_copy(
            part.at[u, pl.ds(at, size)], to, send_sem.at[u // SENT], sem,
            device_id=target, device_id_type=MESH,
        ).start()

    def ring_start(u, axis, size, fwd, fwd_sem, got, got_sem):
        half = size // 2
        up, down = along(axis, 1), along(axis, 3)
        send(u, 2 * size, half, fwd.at[u, 0], fwd_sem, up)
        send(u, 2 * size + half, half, fwd.at[u, 1], fwd_sem, down)
        send(u, size + half, half, got.at[u, 0, pl.ds(half, half)], got_sem, up)
        send(u, 3 * size, half, got.at[u, 1, pl.ds(0, half)], got_sem, down)

    def ring_forward(u, axis, size, fwd, got, got_sem):
        half = size // 2
        up, down = pl.ds(size, half), pl.ds(3 * size + half, half)
        part[u, up] = part[u, up] + fwd[u, 0]
        part[u, down] = part[u, down] + fwd[u, 1]
        to_up, to_down = got.at[u, 0, pl.ds(0, half)], got.at[u, 1, pl.ds(half, half)]
        send(u, size, half, to_up, got_sem, along(axis, 1))
        send(u, 3 * size + half, half, to_down, got_sem, along(axis, 3))

    def ring_end(u, size, got):
        mine = pl.ds(0, size)
        part[u, mine] = part[u, mine] + got[u, 0] + got[u, 1]

    def chunk_arrived(k, what, sem):
        units = pl.ds(EACH * k, EACH)
        pltpu.make_async_remote_copy(
            what.at[units], what.at[units], send_sem.at[0], sem.at[k],
            device_id=partner, device_id_type=MESH,
        ).wait_recv()

    def units_of(k):
        return [EACH * k + j for j in range(EACH)]

    def start1(u):
        ring_start(u, u % 3, 32, fwd1, fwd1_sem.at[u // 2], got1, got1_sem.at[u // EACH])

    def forward1(k, js=range(EACH)):
        for j in js:
            u = EACH * k + j
            if j % 2 == 0:
                pair = fwd1.at[pl.ds(u, 2)]
                pltpu.make_async_remote_copy(
                    pair, pair, send_sem.at[0], fwd1_sem.at[u // 2],
                    device_id=partner, device_id_type=MESH,
                ).wait_recv()
            ring_forward(u, u % 3, 32, fwd1, got1, got1_sem.at[k])

    def start2(k):
        chunk_arrived(k, got1, got1_sem)
        for u in units_of(k):
            ring_end(u, 32, got1)
            ring_start(u, axes_of(u)[1], 8, fwd2, fwd2_sem.at[k], got2, got2_sem.at[k])

    def forward2(k):
        chunk_arrived(k, fwd2, fwd2_sem)
        for u in units_of(k):
            ring_forward(u, axes_of(u)[1], 8, fwd2, got2, got2_sem.at[k])

    def start3(k):
        chunk_arrived(k, got2, got2_sem)
        for u in units_of(k):
            ring_end(u, 8, got2)
            for step in (2, 1, 3):
                to = got3.at[u, step - 1]
                send(u, 2 * step, 2, to, got3_sem.at[k], along(axes_of(u)[2], step))

    def end3(k):
        chunk_arrived(k, got3, got3_sem)
        for u in units_of(k):
            final = part[u, 0:2] + got3[u, 0] + got3[u, 1] + got3[u, 2]
            grad[:, pl.ds(pl.multiple_of(u * W, W), W)] = final.reshape(16, W)
            squares[...] = squares[...] + final * final

    def all_sent(i):
        sent = part.at[pl.ds(SENT * i, SENT), pl.ds(0, 126)]
        pltpu.make_async_remote_copy(
            sent, sent, send_sem.at[i], got3_sem.at[0],
            device_id=partner, device_id_type=MESH,
        ).wait_send()

    def own(k, js=range(EACH)):
        def store(j, place, value):
            part[EACH * k + j, place] = value

        product(k, 1, store, js)

    def exchange_ended(k, j):
        u, slot = EACH * k + j, k % SLOTS
        exchanged(k, j).wait_recv()

        def add(i, carry):
            at = pl.ds(pl.multiple_of(16 * i, 16), 16)
            part[u, at] = part[u, at] + other[slot, j, at]
            return carry

        lax.fori_loop(0, 8, add, 0)
        start1(u)

    low, high = range(2), range(2, 4)
    x_loads[0].wait()
    transposed(0)
    x_loads[2].start()
    x_loads[1].wait()
    c_next.start()
    c_second.start()
    transposed(1)
    x_loads[3].start()
    c_first.wait()
    exchange_product(0, low)
    pl.semaphore_wait(barrier, 22)
    exchange(0, low)
    c_next.wait()
    exchange_product(0, high)
    exchange(0, high)
    x_loads[2].wait()
    transposed(2)
    x_loads[3].wait()
    transposed(3)
    c_second.wait()
    c_rest.start()
    own(0, low)
    exchange_ended(0, 0)
    exchange_ended(0, 1)
    exchange_product(1, low)
    exchange(1, low)
    own(0, high)
    exchange_ended(0, 2)
    exchange_ended(0, 3)
    exchange_product(1, high)
    exchange(1, high)
    own(1, low)
    exchange_ended(1, 0)
    exchange_ended(1, 1)
    c_rest.wait()
    exchange_sent(0)
    exchange_product(2, low)
    exchange(2, low)
    forward1(0, low)
    own(1, high)
    exchange_ended(1, 2)
    exchange_ended(1, 3)
    exchange_product(2, high)
    exchange(2, high)
    forward1(0, high)

    def step(k, carry):
        own(k)
        for j in range(EACH):
            exchange_ended(k, j)

        @pl.when(k == 2)
        def _():
            exchange_sent(1)
            exchange_product(3)
            exchange(3)

        forward1(k - 1)

        @pl.when(k + 2 < CHUNKS)
        def _():
            exchange_sent(k)
            exchange_product(k + 2)
            exchange(k + 2)

        @pl.when(k < 5)
        def _():
            start2(k - 2)

        @pl.when((k >= 4) & (k < 5))
        def _():
            forward2(k - 4)

        return carry

    lax.fori_loop(2, CHUNKS, step, 0)
    exchange_sent(CHUNKS - 2)
    exchange_sent(CHUNKS - 1)

    def all_of(low, high, what):
        if high - low == 1:
            what(low)
            return

        def one_chunk(k, carry):
            what(k)
            return carry

        lax.fori_loop(low, high, one_chunk, 0)

    all_of(7, 8, forward1)
    all_of(3, 6, start2)
    all_of(1, 3, forward2)
    all_of(6, 8, start2)
    all_of(3, 6, forward2)
    all_of(6, 8, forward2)
    all_of(0, 6, start3)
    all_of(6, 8, start3)
    all_of(0, 8, end3)

    total = squares[0] + squares[1]
    for level, (targets, inbox) in enumerate(((column, norm_in1), (plane, norm_in2))):
        norm_out[level] = total
        copies = [
            pltpu.make_async_remote_copy(
                norm_out.at[level], inbox.at[place], norm_send.at[level],
                norm_recv.at[level], device_id=target, device_id_type=MESH,
            )
            for place, target in targets
        ]
        for copy in copies:
            copy.start()
        whole = pltpu.make_async_remote_copy(
            inbox, inbox, norm_send.at[level], norm_recv.at[level],
            device_id=partner, device_id_type=MESH,
        )
        whole.wait_recv()
        for place, _ in targets:
            total = total + inbox[place]
        whole.wait_send()

    limit = 0.5 * jnp.sqrt(jnp.float32(ROWS * D))
    whole = jnp.sum(total, keepdims=True)
    factor = limit / jnp.maximum(jnp.sqrt(whole), limit)
    for i in range(UNITS // SENT):
        all_sent(i)
    scaled_ref[...] = grad[...] * factor


def shards(inputs, cotangent, master, accum):
    vmem, dma = pltpu.VMEM, pltpu.SemaphoreType.DMA
    f32, bf16 = jnp.float32, jnp.bfloat16
    scaled = pl.pallas_call(
        kernel,
        out_shape=vmem((16, D), f32),
        in_specs=[pl.BlockSpec(memory_space=pl.ANY)] * 2,
        out_specs=pl.BlockSpec(memory_space=vmem),
        scratch_shapes=[
            vmem((2, TOKENS, 512), bf16),
            vmem((4, TILE, TOKENS), bf16),
            vmem((TOKENS, D), bf16),
            vmem((2, EACH, 128, 8, W), f32),
            vmem((SLOTS, EACH, 128, 8, W), f32),
            vmem((UNITS, 128, 8, W), f32),
            vmem((UNITS, 2, 16, 8, W), f32),
            vmem((UNITS, 2, 32, 8, W), f32),
            vmem((UNITS, 2, 4, 8, W), f32),
            vmem((UNITS, 2, 8, 8, W), f32),
            vmem((UNITS, 3, 2, 8, W), f32),
            vmem((16, D), f32),
            vmem((2, 8, W), f32),
            vmem((2, 8, W), f32),
            vmem((7, 8, W), f32),
            vmem((15, 8, W), f32),
            dma((4,)),
            dma((4,)),
            dma((2,)),
            dma((SLOTS, EACH)),
            dma((UNITS // SENT,)),
            dma((UNITS // 2,)),
            dma((CHUNKS,)),
            dma((CHUNKS,)),
            dma((CHUNKS,)),
            dma((CHUNKS,)),
            dma((2,)),
            dma((2,)),
        ],
        compiler_params=pltpu.CompilerParams(
            collective_id=0, has_side_effects=True, vmem_limit_bytes=64_000_000
        ),
        name="gradient_sum",
    )(inputs, cotangent)
    new_accum = accum + scaled * scaled
    new_master = master - 0.5 * scaled / jnp.sqrt(new_accum)
    return new_master, new_accum


def solution(mesh):
    rows = P(("gx", "gy", "gz"), None)
    return jax.shard_map(
        shards, mesh=mesh, in_specs=(rows,) * 4, out_specs=(rows, rows), check_vma=False
    )
```

```python
import jax
import jax.numpy as jnp
from jax import lax
from jax.experimental import pallas as pl
from jax.experimental.pallas import tpu as pltpu
from jax.sharding import PartitionSpec as P

MESH = pl.DeviceIdType.MESH

D = 4096
ROWS = 2048
TOKENS = 1024
W = 128
EACH = 4
WIDE = EACH * W
CHUNKS = D // WIDE
UNITS = D // W
TILE = 512
SLOTS = 4
SENT = 8


def one_hot(axis):
    return ((axis + 2) % 3 // 2, (axis + 1) % 3 // 2, axis // 2)


def axes_of(u):
    return u % 3, (u + 1) % 3, (u + 2) % 3


def kernel(
    x_hbm, c_hbm,
    scaled_ref,
    xv, cv, stage, other, part, fwd1, got1, fwd2, got2, got3,
    grad, squares, norm_out, norm_in1, norm_in2,
    x_sem, c_sem, stage_sem, other_sem, send_sem,
    fwd1_sem, got1_sem, fwd2_sem, got2_sem, got3_sem, norm_send, norm_recv,
):
    gx, gy, gz = lax.axis_index("gx"), lax.axis_index("gy"), lax.axis_index("gz")
    core = gx % 2
    me = (gz % 4, 2 * (gx // 2) + gz // 4, gy)

    def device(x, y, z, on):
        return (2 * (y // 2) + on, z, 4 * (y % 2) + x)

    def along(axis, step):
        x, y, z = ((at + step * hot) % 4 for at, hot in zip(me, one_hot(axis)))
        return device(x, y, z, core)

    partner = device(*me, 1 - core)

    x_loads = []
    for j in range(4):
        whose = 1 - core if j < 2 else core
        at = pl.multiple_of((j % 2) * 1024 + whose * 512, 512)
        x_loads.append(
            pltpu.make_async_copy(x_hbm.at[:, pl.ds(at, 512)], xv.at[j], x_sem.at[j])
        )
    c_first, c_next = [
        pltpu.make_async_copy(c_hbm.at[:, at], cv.at[:, at], c_sem.at[i])
        for i, at in ((0, pl.ds(0, 2 * W)), (3, pl.ds(2 * W, 2 * W)))
    ]
    c_second = pltpu.make_async_copy(
        c_hbm.at[:, pl.ds(WIDE, WIDE)], cv.at[:, pl.ds(WIDE, WIDE)], c_sem.at[1]
    )
    rest = pl.ds(2 * WIDE, D - 2 * WIDE)
    c_rest = pltpu.make_async_copy(c_hbm.at[:, rest], cv.at[:, rest], c_sem.at[2])
    x_loads[0].start()
    c_first.start()
    x_loads[1].start()

    column = [
        (3 * on + step - 1, (me[0], me[1], (me[2] + step) % 4), (core + on) % 2)
        for step, on in ((2, 1), (2, 0), (1, 1), (3, 1), (1, 0), (3, 0), (4, 1))
    ]
    column = [(place, device(*at, on)) for place, at, on in column]
    plane = [
        (4 * a + b - 1 - (a > 0), device((me[0] + a) % 4, (me[1] + b) % 4, me[2], core))
        for a in (2, 1, 3, 0)
        for b in (2, 1, 3, 4)
        if (a, b) != (0, 4)
    ]
    barrier = pltpu.get_barrier_semaphore()
    for _, target in column + plane:
        pl.semaphore_signal(barrier, inc=1, device_id=target, device_id_type=MESH)

    squares[...] = jnp.zeros_like(squares)

    def transposed(j):
        pass

    def product(k, own, store, js=range(EACH)):
        at = pl.multiple_of(k * WIDE + js[0] * W, len(js) * W)
        columns = pl.ds(at, len(js) * W)
        hots = [[one_hot(axis) for axis in axes_of(EACH * k + j)] for j in js]
        weights = [
            [32 * a + 8 * b + 2 * c for a, b, c in zip(*of_unit)] for of_unit in hots
        ]

        def tile(m, carry):
            block = lax.dot_general(
                xv[2 * own + m], cv[:, columns], (((0,), (0,)), ((), ())),
                preferred_element_type=jnp.float32,
            )
            for i, j in enumerate(js):
                wx, wy, wz = weights[i]
                xs = [wx * ((to - me[0] + 4) % 4) for to in range(4)]
                ys = [wy * ((2 * m + to - me[1] + 4) % 4) for to in range(2)]
                zs = [wz * ((to - me[2] + 4) % 4) for to in range(4)]
                for b in range(32):
                    place = xs[b % 4] + ys[b // 4 % 2] + zs[b // 8]
                    value = block[16 * b : 16 * b + 16, W * i : W * i + W]
                    store(j, pl.ds(place, 2), value.reshape(2, 8, W))
            return carry

        lax.fori_loop(0, 2, tile, 0, unroll=len(js) < EACH)

    def exchanged(k, j):
        slot, to = k % 2, k % SLOTS
        return pltpu.make_async_remote_copy(
            stage.at[slot, j], other.at[to, j], stage_sem.at[slot], other_sem.at[to, j],
            device_id=partner, device_id_type=MESH,
        )

    def exchange_product(k, js=range(EACH)):
        def store(j, place, value):
            stage[k % 2, j, place] = value

        product(k, 0, store, js)

    def exchange(k, js=range(EACH)):
        for j in js:
            exchanged(k, j).start()

    def exchange_sent(k):
        slot = k % 2
        pltpu.make_async_remote_copy(
            stage.at[slot], other.at[0], stage_sem.at[slot], other_sem.at[0, 0],
            device_id=partner, device_id_type=MESH,
        ).wait_send()

    def send(u, at, size, to, sem, target):
        pltpu.make_async_remote_copy(
            part.at[u, pl.ds(at, size)], to, send_sem.at[u // SENT], sem,
            device_id=target, device_id_type=MESH,
        ).start()

    def ring_start(u, axis, size, fwd, fwd_sem, got, got_sem, now=(0, 1)):
        half = size // 2
        up, down = along(axis, 1), along(axis, 3)
        if 0 in now:
            send(u, 2 * size, half, fwd.at[u, 0], fwd_sem, up)
            send(u, 2 * size + half, half, fwd.at[u, 1], fwd_sem, down)
        if 1 in now:
            send(u, size + half, half, got.at[u, 0, pl.ds(half, half)], got_sem, up)
            send(u, 3 * size, half, got.at[u, 1, pl.ds(0, half)], got_sem, down)

    def ring_forward(u, axis, size, fwd, got, got_sem):
        half = size // 2
        up, down = pl.ds(size, half), pl.ds(3 * size + half, half)
        part[u, up] = part[u, up] + fwd[u, 0]
        part[u, down] = part[u, down] + fwd[u, 1]
        to_up, to_down = got.at[u, 0, pl.ds(0, half)], got.at[u, 1, pl.ds(half, half)]
        send(u, size, half, to_up, got_sem, along(axis, 1))
        send(u, 3 * size + half, half, to_down, got_sem, along(axis, 3))

    def ring_end(u, size, got):
        mine = pl.ds(0, size)
        part[u, mine] = part[u, mine] + got[u, 0] + got[u, 1]

    def chunk_arrived(k, what, sem):
        units = pl.ds(EACH * k, EACH)
        pltpu.make_async_remote_copy(
            what.at[units], what.at[units], send_sem.at[0], sem.at[k],
            device_id=partner, device_id_type=MESH,
        ).wait_recv()

    def units_of(k):
        return [EACH * k + j for j in range(EACH)]

    def start1(u, now=(0, 1)):
        sems = fwd1_sem.at[u // 2], got1_sem.at[u // EACH]
        ring_start(u, u % 3, 32, fwd1, sems[0], got1, sems[1], now)

    def forward1(k, js=range(EACH)):
        for j in js:
            u = EACH * k + j
            if j % 2 == 0:
                pair = fwd1.at[pl.ds(u, 2)]
                pltpu.make_async_remote_copy(
                    pair, pair, send_sem.at[0], fwd1_sem.at[u // 2],
                    device_id=partner, device_id_type=MESH,
                ).wait_recv()
            ring_forward(u, u % 3, 32, fwd1, got1, got1_sem.at[k])

    def start2(k):
        chunk_arrived(k, got1, got1_sem)
        for now in (0, 1):
            for u in units_of(k):
                if now == 0:
                    ring_end(u, 32, got1)
                sems = fwd2_sem.at[k], got2_sem.at[k]
                ring_start(u, axes_of(u)[1], 8, fwd2, sems[0], got2, sems[1], (now,))

    def forward2(k):
        chunk_arrived(k, fwd2, fwd2_sem)
        for u in units_of(k):
            ring_forward(u, axes_of(u)[1], 8, fwd2, got2, got2_sem.at[k])

    def start3(k):
        chunk_arrived(k, got2, got2_sem)
        for u in units_of(k):
            ring_end(u, 8, got2)
            for step in (2, 1, 3):
                to = got3.at[u, step - 1]
                send(u, 2 * step, 2, to, got3_sem.at[k], along(axes_of(u)[2], step))

    def end3(k):
        chunk_arrived(k, got3, got3_sem)
        for u in units_of(k):
            final = part[u, 0:2] + got3[u, 0] + got3[u, 1] + got3[u, 2]
            grad[:, pl.ds(pl.multiple_of(u * W, W), W)] = final.reshape(16, W)
            squares[...] = squares[...] + final * final

    def all_sent(i):
        sent = part.at[pl.ds(SENT * i, SENT), pl.ds(0, 126)]
        pltpu.make_async_remote_copy(
            sent, sent, send_sem.at[i], got3_sem.at[0],
            device_id=partner, device_id_type=MESH,
        ).wait_send()

    def own(k, js=range(EACH)):
        def store(j, place, value):
            part[EACH * k + j, place] = value

        product(k, 1, store, js)

    def exchange_ended(k, j, now=(0, 1)):
        u, slot = EACH * k + j, k % SLOTS
        exchanged(k, j).wait_recv()

        def add(i, carry):
            at = pl.ds(pl.multiple_of(16 * i, 16), 16)
            part[u, at] = part[u, at] + other[slot, j, at]
            return carry

        lax.fori_loop(0, 8, add, 0)
        start1(u, now)

    low, high = range(2), range(2, 4)
    x_loads[0].wait()
    transposed(0)
    x_loads[2].start()
    x_loads[1].wait()
    c_next.start()
    c_second.start()
    transposed(1)
    x_loads[3].start()
    c_first.wait()
    exchange_product(0, low)
    pl.semaphore_wait(barrier, 22)
    exchange(0, low)
    c_next.wait()
    exchange_product(0, high)
    exchange(0, high)
    x_loads[2].wait()
    transposed(2)
    x_loads[3].wait()
    transposed(3)
    c_second.wait()
    c_rest.start()
    own(0, low)
    exchange_ended(0, 0)
    exchange_ended(0, 1)
    exchange_product(1, low)
    exchange(1, low)
    own(0, high)
    exchange_ended(0, 2)
    exchange_ended(0, 3)
    exchange_product(1, high)
    exchange(1, high)
    own(1, low)
    exchange_ended(1, 0)
    exchange_ended(1, 1)
    c_rest.wait()
    exchange_sent(0)
    exchange_product(2, low)
    exchange(2, low)
    forward1(0, low)
    own(1, high)
    exchange_ended(1, 2)
    exchange_ended(1, 3)
    exchange_product(2, high)
    exchange(2, high)
    forward1(0, high)

    def step(k, carry):
        own(k)
        for j in range(EACH):
            exchange_ended(k, j, (0,))
        for j in range(EACH):
            start1(EACH * k + j, (1,))

        @pl.when(k == 2)
        def _():
            exchange_sent(1)
            exchange_product(3)
            exchange(3)

        forward1(k - 1)

        @pl.when(k + 2 < CHUNKS)
        def _():
            exchange_sent(k)
            exchange_product(k + 2)
            exchange(k + 2)

        @pl.when(k < 5)
        def _():
            start2(k - 2)

        @pl.when((k >= 4) & (k < 5))
        def _():
            forward2(k - 4)

        return carry

    lax.fori_loop(2, CHUNKS, step, 0)
    exchange_sent(CHUNKS - 2)
    exchange_sent(CHUNKS - 1)

    def all_of(low, high, what):
        if high - low == 1:
            what(low)
            return

        def one_chunk(k, carry):
            what(k)
            return carry

        lax.fori_loop(low, high, one_chunk, 0)

    all_of(7, 8, forward1)
    all_of(3, 6, start2)
    all_of(1, 3, forward2)
    all_of(6, 8, start2)
    all_of(3, 6, forward2)
    all_of(6, 8, forward2)
    all_of(0, 6, start3)
    all_of(6, 8, start3)
    all_of(0, 8, end3)

    total = squares[0] + squares[1]
    for level, (targets, inbox) in enumerate(((column, norm_in1), (plane, norm_in2))):
        norm_out[level] = total
        copies = [
            pltpu.make_async_remote_copy(
                norm_out.at[level], inbox.at[place], norm_send.at[level],
                norm_recv.at[level], device_id=target, device_id_type=MESH,
            )
            for place, target in targets
        ]
        for copy in copies:
            copy.start()
        whole = pltpu.make_async_remote_copy(
            inbox, inbox, norm_send.at[level], norm_recv.at[level],
            device_id=partner, device_id_type=MESH,
        )
        whole.wait_recv()
        for place, _ in targets:
            total = total + inbox[place]
        whole.wait_send()

    limit = 0.5 * jnp.sqrt(jnp.float32(ROWS * D))
    whole = jnp.sum(total, keepdims=True)
    factor = limit / jnp.maximum(jnp.sqrt(whole), limit)
    for i in range(UNITS // SENT):
        all_sent(i)
    scaled_ref[...] = grad[...] * factor


def shards(inputs, cotangent, master, accum):
    vmem, dma = pltpu.VMEM, pltpu.SemaphoreType.DMA
    f32, bf16 = jnp.float32, jnp.bfloat16
    scaled = pl.pallas_call(
        kernel,
        out_shape=vmem((16, D), f32),
        in_specs=[pl.BlockSpec(memory_space=pl.ANY)] * 2,
        out_specs=pl.BlockSpec(memory_space=vmem),
        scratch_shapes=[
            vmem((4, TOKENS, 512), bf16),
            vmem((TOKENS, D), bf16),
            vmem((2, EACH, 128, 8, W), f32),
            vmem((SLOTS, EACH, 128, 8, W), f32),
            vmem((UNITS, 128, 8, W), f32),
            vmem((UNITS, 2, 16, 8, W), f32),
            vmem((UNITS, 2, 32, 8, W), f32),
            vmem((UNITS, 2, 4, 8, W), f32),
            vmem((UNITS, 2, 8, 8, W), f32),
            vmem((UNITS, 3, 2, 8, W), f32),
            vmem((16, D), f32),
            vmem((2, 8, W), f32),
            vmem((2, 8, W), f32),
            vmem((7, 8, W), f32),
            vmem((15, 8, W), f32),
            dma((4,)),
            dma((4,)),
            dma((2,)),
            dma((SLOTS, EACH)),
            dma((UNITS // SENT,)),
            dma((UNITS // 2,)),
            dma((CHUNKS,)),
            dma((CHUNKS,)),
            dma((CHUNKS,)),
            dma((CHUNKS,)),
            dma((2,)),
            dma((2,)),
        ],
        compiler_params=pltpu.CompilerParams(
            collective_id=0, has_side_effects=True, vmem_limit_bytes=64_000_000
        ),
        name="gradient_sum",
    )(inputs, cotangent)
    new_accum = accum + scaled * scaled
    new_master = master - 0.5 * scaled / jnp.sqrt(new_accum)
    return new_master, new_accum


def solution(mesh):
    rows = P(("gx", "gy", "gz"), None)
    return jax.shard_map(
        shards, mesh=mesh, in_specs=(rows,) * 4, out_specs=(rows, rows), check_vma=False
    )
```
